32 devices in a mesh: dp: 8 (over z, y), mp: 4 (over x, core).
Axes of the slice: x: 2, y: 2, z: 4, core: 2. Of those that a mesh axis runs over, the one named last changes fastest.
Arguments:
- patches: bfloat16 [192, 256, 768], P('dp'), may hold values from -6 to 6
- keep_index: int32 [192, 64], P('dp'), may hold values from 0 to 255, as said below
- ln1_gain: float32 [768], replicated, may hold values from 0.1 to 1.9
- ln1_bias: float32 [768], replicated, may hold values from -2 to 2
- qkv_weight: bfloat16 [768, 3, 768], P(None, None, 'mp'), may hold values from -0.21875 to 0.21875
- qkv_bias: float32 [3, 768], P(None, 'mp'), may hold values from -2 to 2
- proj_weight: bfloat16 [768, 768], P('mp'), may hold values from -0.625 to 0.625
- proj_bias: float32 [768], replicated, may hold values from -2 to 2
- ln2_gain: float32 [768], replicated, may hold values from 0.1 to 1.9
- ln2_bias: float32 [768], replicated, may hold values from -2 to 2
- up_weight: bfloat16 [768, 3072], P(None, 'mp'), may hold values from -0.21875 to 0.21875
- up_bias: float32 [3072], P('mp'), may hold values from -2 to 2
- down_weight: bfloat16 [3072, 768], P('mp'), may hold values from -0.109375 to 0.109375
- down_bias: float32 [768], replicated, may hold values from -2 to 2
- out_grad: bfloat16 [192, 64, 768], P('dp'), may hold values from -6 to 6
Outputs:
- layer_out: bfloat16 [192, 64, 768], P('dp')
- patches_grad: bfloat16 [192, 256, 768], P('dp')
- ln1_gain_grad: float32 [768], replicated
- ln1_bias_grad: float32 [768], replicated
- qkv_weight_grad: float32 [768, 3, 768], P('dp', None, 'mp')
- qkv_bias_grad: float32 [3, 768], P(None, 'mp')
- proj_weight_grad: float32 [768, 768], P('mp', 'dp')
- proj_bias_grad: float32 [768], replicated
- ln2_gain_grad: float32 [768], replicated
- ln2_bias_grad: float32 [768], replicated
- up_weight_grad: float32 [768, 3072], P('dp', 'mp')
- up_bias_grad: float32 [3072], P('mp')
- down_weight_grad: float32 [3072, 768], P('mp', 'dp')
- down_bias_grad: float32 [768], replicated
The draws below stay inside these ranges and needn't reach their ends.
Inputs may be any that keep to these rules, and one draw needn't show every extreme that they name: `keep_index`: each item's 64 indices are distinct and rise.
All inputs are finite; a program needn't handle non-finite values.
Results may differ from the reference program's by a relative error of at most 0.018.
Values may be sent and summed in bfloat16 or wider, within the bound.
A program may use at most 128 MiB of HBM per device.

```python
import jax
import jax.numpy as jnp
from jax import lax

D = 768
H = 12
HD = 64
FF = 3072
PATCHES = 256
VIS = 64
ITEM_DEV = 24
ITEMS = 192
N_DP = 8


def draw_keep_index(key, part):
    item_keys = jax.random.split(jax.random.fold_in(key, 17), ITEMS)

    def one_item(item_key):
        return jnp.sort(jax.random.permutation(item_key, PATCHES)[:VIS])
    return jax.vmap(one_item)(item_keys).astype(jnp.int32)


def shard_levels(rng, dims, cuts, smallest, top_value):
    level, own = 1.0, jax.random.fold_in(rng, 6)
    for axis_at, blocks in cuts:
        steps = jnp.exp(jax.random.uniform(jax.random.fold_in(own, axis_at), (blocks,), jnp.float32, smallest / len(cuts), top_value / len(cuts)))
        level = level * jnp.repeat(steps, dims[axis_at] // blocks).reshape([-1 if axis == axis_at else 1 for axis in range(len(dims))])
    return level


def gaussian(own_key, shape, scale, reach, cuts=(), dtype=jnp.bfloat16):
    result = jax.random.normal(own_key, shape, jnp.float32) * scale
    if len(cuts) > 0:
        result = shard_levels(own_key, shape, cuts, -0.22, 0.18) * result
    return jnp.clip(result, min=-reach, max=reach).astype(dtype)


def setup_inputs(seed: int = 0) -> dict:
    key_list = jax.random.split(jax.random.key(seed), 16)
    patches = gaussian(key_list[0], (ITEMS, PATCHES, D), 1.0, 6.0, ((0, 8),))
    keep_index = draw_keep_index(jax.random.fold_in(key_list[15], 71), 0)
    ln1_gain = jnp.clip(1.0 + 0.18 * jax.random.normal(key_list[2], (D,), jnp.float32), 0.1, 1.9)
    ln1_bias = gaussian(key_list[3], (D,), 0.3, 2.0, (), jnp.float32)
    qkv_weight = gaussian(key_list[4], (D, 3, D), D ** -0.5, 0.21875, ((2, 4),))
    qkv_bias = gaussian(key_list[5], (3, D), 0.3, 2.0, ((1, 4),), jnp.float32)
    proj_weight = gaussian(key_list[6], (D, D), (D // 8) ** -0.5, 0.625, ((0, 4),))
    proj_bias = gaussian(key_list[7], (D,), 0.3, 2.0, (), jnp.float32)
    ln2_gain = jnp.clip(1.0 + 0.18 * jax.random.normal(key_list[8], (D,), jnp.float32), 0.1, 1.9)
    ln2_bias = gaussian(key_list[9], (D,), 0.3, 2.0, (), jnp.float32)
    up_weight = gaussian(key_list[10], (D, FF), D ** -0.5, 0.21875, ((1, 4),))
    up_bias = gaussian(key_list[11], (FF,), 0.3, 2.0, ((0, 4),), jnp.float32)
    down_weight = gaussian(key_list[12], (FF, D), FF ** -0.5, 0.109375, ((0, 4),))
    down_bias = gaussian(key_list[13], (D,), 0.3, 2.0, (), jnp.float32)
    out_grad = gaussian(key_list[14], (ITEMS, VIS, D), 1.0, 6.0, ((0, 8),))
    return {"patches": patches, "keep_index": keep_index, "ln1_gain": ln1_gain, "ln1_bias": ln1_bias, "qkv_weight": qkv_weight, "qkv_bias": qkv_bias, "proj_weight": proj_weight, "proj_bias": proj_bias, "ln2_gain": ln2_gain, "ln2_bias": ln2_bias, "up_weight": up_weight, "up_bias": up_bias, "down_weight": down_weight, "down_bias": down_bias, "out_grad": out_grad}


EPSILON = 1e-05
HIGH = lax.Precision.HIGHEST

@jax.custom_vjp
def low(v):
    return lax.optimization_barrier(v.astype(jnp.bfloat16)).astype(jnp.float32)

@jax.custom_vjp
def low_back(v):
    return v

def low_keep(v):
    return (low(v), None)

def low_pass(kept, grad):
    return (grad,)

def back_keep(v):
    return (v, None)

def back_low(kept, grad):
    return (low(grad),)
low.defvjp(low_keep, low_pass)
low_back.defvjp(back_keep, back_low)

def layer_norm(rows, gain, bias):
    centre = rows - lax.optimization_barrier(jnp.mean(rows, axis=-1, keepdims=True))
    spread = lax.optimization_barrier(jnp.mean(centre * centre, axis=-1, keepdims=True))
    return centre * lax.rsqrt(spread + EPSILON) * gain + bias

def gelu_exact(values):
    return 0.5 * values * (1.0 + jax.scipy.special.erf(values * 0.7071067811865476))

def layer_forward(keep_index, patches, ln1_gain, ln1_bias, qkv_weight, qkv_bias, proj_weight, proj_bias, ln2_gain, ln2_bias, up_weight, up_bias, down_weight, down_bias):
    items = patches.shape[0]
    tokens = jnp.take_along_axis(patches, keep_index[:, :, None], axis=1).reshape(items * VIS, D)
    normed_first = low(layer_norm(tokens, ln1_gain, ln1_bias))
    qkv = jnp.dot(normed_first, qkv_weight.reshape(D, 3 * D), precision=HIGH) + qkv_bias.reshape(-1)
    qkv = low(low_back(qkv)).reshape(items, VIS, 3, H, HD)
    queries = qkv[:, :, 0]
    keys = qkv[:, :, 1]
    values = qkv[:, :, 2]
    scores = low_back(jnp.einsum('ivhd,iwhd->ihvw', queries, keys, precision=HIGH) * 0.125)
    probs = low(jax.nn.softmax(scores, axis=-1))
    context = jnp.einsum('ihvw,iwhd->ivhd', probs, values, precision=HIGH)
    context = low(low_back(context)).reshape(items * VIS, D)
    attn = low_back(jnp.dot(context, proj_weight, precision=HIGH)) + proj_bias
    hidden_in = tokens + attn
    normed_second = low(layer_norm(hidden_in, ln2_gain, ln2_bias))
    pre_act = low_back(jnp.dot(normed_second, up_weight, precision=HIGH) + up_bias)
    act = low(gelu_exact(pre_act))
    mlp_out = jnp.dot(act, down_weight, precision=HIGH) + down_bias
    return (hidden_in + mlp_out).reshape(items, VIS, D)

def reference(patches, keep_index, ln1_gain, ln1_bias, qkv_weight, qkv_bias, proj_weight, proj_bias, ln2_gain, ln2_bias, up_weight, up_bias, down_weight, down_bias, out_grad):
    params = (ln1_gain.astype(jnp.float32), ln1_bias.astype(jnp.float32), qkv_weight.astype(jnp.float32), qkv_bias.astype(jnp.float32), proj_weight.astype(jnp.float32), proj_bias.astype(jnp.float32), ln2_gain.astype(jnp.float32), ln2_bias.astype(jnp.float32), up_weight.astype(jnp.float32), up_bias.astype(jnp.float32), down_weight.astype(jnp.float32), down_bias.astype(jnp.float32))
    patch_groups = patches.astype(jnp.float32).reshape(N_DP, ITEM_DEV, PATCHES, D)
    keep_groups = keep_index.astype(jnp.int32).reshape(N_DP, ITEM_DEV, VIS)
    grad_groups = out_grad.astype(jnp.float32).reshape(N_DP, ITEM_DEV, VIS, D)

    def group_step(totals, inputs):
        patch_block, keep_block, grad_block = inputs

        def forward_here(patch_rows, *weights):
            return layer_forward(keep_block, patch_rows, *weights)
        outputs, pullback = jax.vjp(forward_here, patch_block, *params)
        grads = pullback(grad_block)
        updated = tuple((total + grad for total, grad in zip(totals, grads[1:])))
        return (updated, (outputs.astype(jnp.bfloat16), grads[0].astype(jnp.bfloat16)))
    initial = tuple((jnp.zeros_like(weight) for weight in params))
    totals, stacked = lax.scan(group_step, initial, (patch_groups, keep_groups, grad_groups))
    layer_out = stacked[0].reshape(ITEMS, VIS, D)
    patches_grad = stacked[1].reshape(ITEMS, PATCHES, D)
    return (layer_out, patches_grad, totals[0], totals[1], totals[2], totals[3], totals[4], totals[5], totals[6], totals[7], totals[8], totals[9], totals[10], totals[11])
```

```python
import functools

import jax
import jax.numpy as jnp
from jax import lax
from jax.experimental import pallas as pl
from jax.experimental.pallas import tpu as pltpu
from jax.sharding import PartitionSpec as P

HD = 64
EPSILON = 1e-05
SQRT_HALF = 0.7071067811865476
INV_ROOT_TWO_PI = 0.3989422804014327
F32 = jnp.float32
BF16 = jnp.bfloat16
CHUNKS = 2
LIMIT = 60 * 1024 * 1024


def mm(a, b):
    return jnp.dot(a, b, preferred_element_type=F32)


def mm_nt(a, b):
    return lax.dot_general(a, b, (((1,), (1,)), ((), ())), preferred_element_type=F32)


def mm_tn(a, b):
    return lax.dot_general(a, b, (((0,), (0,)), ((), ())), preferred_element_type=F32)


def hat_of(rows):
    centre = rows - jnp.mean(rows, axis=-1, keepdims=True)
    inv_std = lax.rsqrt(jnp.mean(centre * centre, axis=-1, keepdims=True) + EPSILON)
    return centre * inv_std, inv_std


def norm_back(grad_out, hat_rows, inv_std, gain):
    grad_hat = grad_out * gain
    first = jnp.mean(grad_hat, axis=-1, keepdims=True)
    second = jnp.mean(grad_hat * hat_rows, axis=-1, keepdims=True)
    return inv_std * (grad_hat - first - hat_rows * second)


def head_masks():
    lane = lax.broadcasted_iota(jnp.int32, (2 * HD, 2 * HD), 1)
    one = (lane < HD).astype(F32).astype(BF16)
    return one, (lane >= HD).astype(F32).astype(BF16)


def split_heads(pair, masks):
    return jnp.concatenate([pair * masks[0], pair * masks[1]], axis=0)


def head_kernel(core, patches, keep, gain, bias, wqkv, bqkv, proj, tok, normed, qkv, probs, ctx, part):
    items, patch_count = patches.shape[0], patches.shape[1]
    visible = keep.shape[2]
    for i in range(items):
        rows = slice(i * visible, (i + 1) * visible)
        where_row = lax.broadcasted_iota(jnp.int32, (patch_count, visible), 0)
        chosen = (where_row == keep[0, i : i + 1, :]).astype(F32).astype(BF16)
        token = mm_tn(chosen, patches[i])
        tok[rows, :] = token.astype(BF16)
        hat, _ = hat_of(token)
        normed[rows, :] = (hat * gain[...] + bias[...]).astype(BF16)
    for j in range(3):
        qkv[j] = (mm(normed[...], wqkv[j]) + bqkv[j : j + 1, :]).astype(BF16)
    masks = head_masks()
    row_item = (lax.broadcasted_iota(jnp.int32, (4 * HD, 2 * HD), 0) // visible) % 2
    own = row_item == lax.broadcasted_iota(jnp.int32, (4 * HD, 2 * HD), 1) // visible
    pairs = proj.shape[0] // (2 * HD)

    def two_items(p, _):
        rows = pl.ds(pl.multiple_of(p * 2 * visible, 2 * visible), 2 * visible)
        for h in range(pairs):
            cols = slice(h * 2 * HD, (h + 1) * 2 * HD)
            query, key, value = qkv[0, rows, cols], qkv[1, rows, cols], qkv[2, rows, cols]
            scores = mm_nt(split_heads(query, masks), key) * 0.125
            scores = jnp.where(own, scores, -1e30)
            top = jnp.max(scores, axis=-1, keepdims=True)
            e = jnp.where(own, jnp.exp(scores - top), 0.0)
            low = (e * (1.0 / jnp.sum(e, axis=-1, keepdims=True))).astype(BF16)
            probs[p * pairs + h] = low
            wide = jnp.concatenate([low[: 2 * visible], low[2 * visible :]], axis=1)
            ctx[rows, cols] = mm(wide, split_heads(value, masks)).astype(BF16)
        return 0

    lax.fori_loop(0, items // 2, two_items, 0)
    part[...] = mm(ctx[...], proj[...]).astype(BF16)


def mlp_kernel(
    core, tok, part, recv, proj_bias, gain, bias, up_m, up_p, upb, down_m, down_p, og,
    hidden, normed, act, pre_grad, mlp_part, norm_part, upb_sum, mlp_acc, norm_acc,
):
    rows = tok[...].astype(F32) + (part[...].astype(F32) + recv[...].astype(F32)) + proj_bias[...]
    hidden[...] = rows
    hat, _ = hat_of(rows)
    normed[...] = (hat * gain[...] + bias[...]).astype(BF16)
    mlp_acc[...] = jnp.zeros_like(mlp_acc)
    norm_acc[...] = jnp.zeros_like(norm_acc)
    units = up_m.shape[1]
    width = 256

    def block(b, _):
        for side, (up, down) in enumerate(((up_m, down_m), (up_p, down_p))):
            at = pl.multiple_of(b * width, width)
            here = pl.ds(at, width)
            there = pl.ds(pl.multiple_of(side * units + at, width), width)
            up_block = up[:, here]
            down_block = down[here, :]
            pre = mm(normed[...], up_block) + upb[:, there]
            cdf = 0.5 * (1.0 + lax.erf(pre * SQRT_HALF))
            low = (pre * cdf).astype(BF16)
            act[:, there] = low
            mlp_acc[...] += mm(low, down_block)
            slope = cdf + pre * (jnp.exp(-0.5 * pre * pre) * INV_ROOT_TWO_PI)
            grad = (mm_nt(og[...], down_block) * slope).astype(BF16)
            pre_grad[:, there] = grad
            upb_sum[:, there] = jnp.sum(grad.astype(F32), axis=0, keepdims=True)
            norm_acc[...] += mm_nt(grad, up_block)
        return 0

    lax.fori_loop(0, units // width, block, 0)
    mlp_part[...] = mlp_acc[...].astype(BF16)
    norm_part[...] = norm_acc[...].astype(BF16)


def back_kernel(
    core, og, hidden, part, recv, gain, proj, probs, qkv, wqkv,
    hidden_grad, hidden_low, qkv_grad, norm_part, sums, qkvb_sum, cg,
):
    visible = HD
    grads = og[...].astype(F32)
    norm_grad = part[...].astype(F32) + recv[...].astype(F32)
    hat, inv = hat_of(hidden[...])
    total = grads + norm_back(norm_grad, hat, inv, gain[...])
    hidden_grad[...] = total
    hidden_low[...] = total.astype(BF16)
    sums[0:1, :] = jnp.sum(norm_grad * hat, axis=0, keepdims=True)
    sums[1:2, :] = jnp.sum(norm_grad, axis=0, keepdims=True)
    sums[2:3, :] = jnp.sum(total, axis=0, keepdims=True)
    sums[3:4, :] = jnp.sum(grads, axis=0, keepdims=True)
    cg[...] = mm_nt(hidden_low[...], proj[...]).astype(BF16)
    masks = head_masks()
    pairs = proj.shape[0] // (2 * HD)

    def two_items(p, _):
        rows = pl.ds(pl.multiple_of(p * 2 * visible, 2 * visible), 2 * visible)
        for h in range(pairs):
            cols = slice(h * 2 * HD, (h + 1) * 2 * HD)
            query, key, value = qkv[0, rows, cols], qkv[1, rows, cols], qkv[2, rows, cols]
            low = probs[p * pairs + h]
            cgs = split_heads(cg[rows, cols], masks)
            prob = low.astype(F32)
            prob_grad = mm_nt(cgs, value)
            dot = jnp.sum(prob * prob_grad, axis=-1, keepdims=True)
            score = (prob * (prob_grad - dot)).astype(BF16)
            wide = jnp.concatenate([score[: 2 * visible], score[2 * visible :]], axis=1)
            qkv_grad[0, rows, cols] = (mm(wide, split_heads(key, masks)) * 0.125).astype(BF16)
            qkv_grad[1, rows, cols] = (mm_tn(score, split_heads(query, masks)) * 0.125).astype(BF16)
            qkv_grad[2, rows, cols] = mm_tn(low, cgs).astype(BF16)
        return 0

    lax.fori_loop(0, og.shape[0] // (2 * visible), two_items, 0)
    acc = mm_nt(qkv_grad[0], wqkv[0])
    acc += mm_nt(qkv_grad[1], wqkv[1])
    acc += mm_nt(qkv_grad[2], wqkv[2])
    norm_part[...] = acc.astype(BF16)
    for j in range(3):
        qkvb_sum[j : j + 1, :] = jnp.sum(qkv_grad[j].astype(F32), axis=0, keepdims=True)


def token_kernel(tok, hidden_grad, part, recv, gain, token_low, sums):
    norm_grad = part[...].astype(F32) + recv[...].astype(F32)
    hat, inv = hat_of(tok[...].astype(F32))
    token_low[...] = (hidden_grad[...] + norm_back(norm_grad, hat, inv, gain[...])).astype(BF16)
    sums[0:1, :] = jnp.sum(norm_grad * hat, axis=0, keepdims=True)
    sums[1:2, :] = jnp.sum(norm_grad, axis=0, keepdims=True)


def scatter_kernel(core, keep, mine, other, out_mine, out_other, grad, layer, *, half):
    item = pl.program_id(0)
    is_mine = (item // half) == core[0]
    patch_count, visible = grad.shape[1], mine.shape[0]
    where_row = lax.broadcasted_iota(jnp.int32, (patch_count, visible), 0)
    chosen = (where_row == keep[0]).astype(F32).astype(BF16)

    @pl.when(is_mine)
    def _():
        grad[0] = mm(chosen, mine[...]).astype(BF16)
        layer[0] = out_mine[...]

    @pl.when(jnp.logical_not(is_mine))
    def _():
        grad[0] = mm(chosen, other[...]).astype(BF16)
        layer[0] = out_other[...]


def grad_kernel(a0, a1, b0, b1, out):
    out[...] = (mm_tn(a0[...], b0[...]) + mm_tn(a1[...], b1[...])).astype(BF16)


def full(shape):
    return pl.BlockSpec(shape, lambda *_: (0,) * len(shape))


def params():
    return pltpu.CompilerParams(vmem_limit_bytes=LIMIT)


def cost(flops, data):
    return pl.CostEstimate(flops=int(flops), bytes_accessed=int(data), transcendentals=0)


def weight_grad(a, b, width, name):
    rows, depth = a[0].shape
    columns = b[0].shape[1]
    return pl.pallas_call(
        grad_kernel,
        grid=(columns // width,),
        in_specs=[full((rows, depth))] * 2 + [pl.BlockSpec((rows, width), lambda i: (0, i))] * 2,
        out_specs=pl.BlockSpec((depth, width), lambda i: (0, i)),
        out_shape=jax.ShapeDtypeStruct((depth, columns), BF16),
        compiler_params=params(),
        cost_estimate=cost(4 * rows * depth * columns, 2 * depth * columns + 4 * rows * (depth + columns)),
        name=name,
    )(*a, *b)


def sum_kernel(x, out, held, send_sem, recv_sem, *, dp_bits):
    mp, dp = lax.axis_index("mp"), lax.axis_index("dp")
    partners = [(dp, mp + 1 - 2 * (mp % 2))]
    for bit in range(dp_bits):
        step = 1 << bit
        partners.append((dp + step - 2 * step * ((dp // step) % 2), mp))
    barrier = pltpu.get_barrier_semaphore()
    for partner in partners:
        pl.semaphore_signal(barrier, inc=1, device_id=partner, device_id_type=pl.DeviceIdType.MESH)
    pl.semaphore_wait(barrier, len(partners))
    held[0] = x[...]
    for at, partner in enumerate(partners):
        copy = pltpu.make_async_remote_copy(
            src_ref=held.at[2 * at],
            dst_ref=held.at[2 * at + 1],
            send_sem=send_sem.at[at],
            recv_sem=recv_sem.at[at],
            device_id=partner,
            device_id_type=pl.DeviceIdType.MESH,
        )
        copy.start()
        copy.wait()
        total = held[2 * at] + held[2 * at + 1]
        if at + 1 < len(partners):
            held[2 * at + 2] = total
        else:
            out[...] = total


def small_sums(x, dp_bits):
    rounds = dp_bits + 1
    return pl.pallas_call(
        functools.partial(sum_kernel, dp_bits=dp_bits),
        out_shape=jax.ShapeDtypeStruct(x.shape, x.dtype),
        in_specs=[pl.BlockSpec(memory_space=pltpu.VMEM)],
        out_specs=pl.BlockSpec(memory_space=pltpu.VMEM),
        scratch_shapes=[
            pltpu.VMEM((2 * rounds,) + x.shape, x.dtype),
            pltpu.SemaphoreType.DMA((rounds,)),
            pltpu.SemaphoreType.DMA((rounds,)),
        ],
        compiler_params=pltpu.CompilerParams(collective_id=0, has_side_effects=True),
        name="small_sums",
    )(x)


def local(
    patches, keep_index, ln1_gain, ln1_bias, qkv_weight, qkv_bias, proj_weight, proj_bias,
    ln2_gain, ln2_bias, up_weight, up_bias, down_weight, down_bias, out_grad,
    *, dp_count, mp_count,
):
    n_items, visible, width = out_grad.shape
    heads_width = qkv_weight.shape[2]
    units = up_weight.shape[1]
    half = n_items // 2
    items = half // CHUNKS
    rows = items * visible
    patch_count = patches.shape[1]
    mp_index = lax.axis_index("mp")
    dp_index = lax.axis_index("dp")
    core = mp_index % 2
    core_arr = core.reshape(1).astype(jnp.int32)
    to_core = [(i, i ^ 1) for i in range(mp_count)]
    to_x = [(i, i ^ 2) for i in range(mp_count)]
    dp_bits = dp_count.bit_length() - 1

    def swap(value):
        return lax.ppermute(value, "mp", to_core)

    def cross(value):
        return lax.ppermute(value, "mp", to_x)

    small = jnp.concatenate([qkv_bias.reshape(-1), up_bias])
    small_other = swap(small)
    own_qkv = jnp.transpose(qkv_weight, (1, 0, 2))
    wqkv = jnp.concatenate([own_qkv, swap(own_qkv)], axis=2)
    proj = jnp.concatenate([proj_weight, swap(proj_weight)], axis=0)
    up_other = swap(up_weight)
    down_other = swap(down_weight)
    n_qkvb = 3 * heads_width
    bqkv = jnp.concatenate([qkv_bias, small_other[:n_qkvb].reshape(3, heads_width)], axis=1)
    upb = jnp.concatenate([up_bias, small_other[n_qkvb:]])[None, :]
    chip_width = 2 * heads_width
    chip_units = 2 * units
    g1, b1, g2, b2 = (v[None, :] for v in (ln1_gain, ln1_bias, ln2_gain, ln2_bias))
    pb = proj_bias[None, :]
    keep_chunks = keep_index.reshape(n_items // items, items, visible)
    grad_flat = out_grad.reshape(n_items * visible, width)
    blocks = (items // 2) * (chip_width // (2 * HD))

    def sds(shape, dtype):
        return jax.ShapeDtypeStruct(shape, dtype)

    def call(kernel, name, in_specs, outs, scratch, estimate, *args):
        return pl.pallas_call(
            kernel,
            grid_spec=pltpu.PrefetchScalarGridSpec(
                num_scalar_prefetch=1,
                grid=(1,),
                in_specs=in_specs,
                out_specs=[full(o.shape) for o in outs],
                scratch_shapes=scratch,
            ),
            out_shape=outs,
            compiler_params=params(),
            cost_estimate=estimate,
            name=name,
        )(core_arr, *args)

    def forward_head(c):
        return call(
            head_kernel, f"head{c}",
            [
                pl.BlockSpec((items, patch_count, width), lambda i, s: (s[0] * CHUNKS + c, 0, 0)),
                pl.BlockSpec((1, items, visible), lambda i, s: (s[0] * CHUNKS + c, 0, 0)),
                full((1, width)), full((1, width)), full(wqkv.shape), full(bqkv.shape), full(proj.shape),
            ],
            [
                sds((rows, width), BF16), sds((rows, width), BF16), sds((3, rows, chip_width), BF16),
                sds((blocks, 4 * HD, 2 * HD), BF16), sds((rows, chip_width), BF16), sds((rows, width), BF16),
            ],
            [], cost(4 * rows * width * 4 * chip_width, 12e6),
            patches, keep_chunks, g1, b1, wqkv, bqkv, proj,
        )

    og_spec = [pl.BlockSpec((rows, width), lambda i, s, c=c: (s[0] * CHUNKS + c, 0)) for c in range(CHUNKS)]

    def mlp(c, tok, part, recv):
        row_spec = full((rows, width))
        return call(
            mlp_kernel, f"mlp{c}",
            [row_spec, row_spec, row_spec, full((1, width)), full((1, width)), full((1, width)),
             full(up_weight.shape), full(up_weight.shape), full(upb.shape),
             full(down_weight.shape), full(down_weight.shape), og_spec[c]],
            [
                sds((rows, width), F32), sds((rows, width), BF16), sds((rows, chip_units), BF16),
                sds((rows, chip_units), BF16), sds((rows, width), BF16), sds((rows, width), BF16),
                sds((1, chip_units), F32),
            ],
            [pltpu.VMEM((rows, width), F32)] * 2, cost(16 * rows * width * chip_units, 20e6),
            tok, part, recv, pb, g2, b2, up_weight, up_other, upb, down_weight, down_other, grad_flat,
        )

    def back(c, hidden, part, recv, probs, qkv):
        row_spec = full((rows, width))
        return call(
            back_kernel, f"back{c}",
            [og_spec[c], row_spec, row_spec, row_spec, full((1, width)), full(proj.shape),
             full(probs.shape), full(qkv.shape), full(wqkv.shape)],
            [
                sds((rows, width), F32), sds((rows, width), BF16), sds((3, rows, chip_width), BF16),
                sds((rows, width), BF16), sds((8, width), F32), sds((3, chip_width), F32),
            ],
            [pltpu.VMEM((rows, chip_width), BF16)], cost(6 * rows * width * 4 * chip_width, 12e6),
            grad_flat, hidden, part, recv, g2, proj, probs, qkv, wqkv,
        )

    def token_grad(c, tok, hidden_grad, part, recv):
        return pl.pallas_call(
            token_kernel,
            out_shape=[sds((rows, width), BF16), sds((8, width), F32)],
            compiler_params=params(),
            cost_estimate=cost(rows * width * 8, 4e6),
            name=f"token{c}",
        )(tok, hidden_grad, part, recv, g1)

    both = range(CHUNKS)
    heads = [forward_head(c) for c in both]
    attn_recv = [cross(h[5]) for h in heads]
    mlps = [mlp(c, heads[c][0], heads[c][5], attn_recv[c]) for c in both]
    norm2_recv = [cross(m[5]) for m in mlps]
    mlp_recv = [cross(m[4]) for m in mlps]
    backs = [back(c, mlps[c][0], mlps[c][5], norm2_recv[c], heads[c][3], heads[c][2]) for c in both]
    norm1_recv = [cross(b[3]) for b in backs]
    tails = [token_grad(c, heads[c][0], backs[c][0], backs[c][3], norm1_recv[c]) for c in both]

    layer_rows = jnp.concatenate(
        [
            (
                mlps[c][0] + (mlps[c][4].astype(F32) + mlp_recv[c].astype(F32)) + down_bias
            ).astype(BF16)
            for c in both
        ],
        axis=0,
    )
    layer_other = swap(layer_rows)
    token_rows = jnp.concatenate([t[0] for t in tails], axis=0)
    token_other = swap(token_rows)
    keep_rows = keep_index.reshape(n_items, 1, visible)
    item_rows = pl.BlockSpec((visible, width), lambda i, s: (i % half, 0))
    patches_grad, layer_out = pl.pallas_call(
        functools.partial(scatter_kernel, half=half),
        grid_spec=pltpu.PrefetchScalarGridSpec(
            num_scalar_prefetch=1,
            grid=(n_items,),
            in_specs=[pl.BlockSpec((1, 1, visible), lambda i, s: (i, 0, 0))] + [item_rows] * 4,
            out_specs=[
                pl.BlockSpec((1, patch_count, width), lambda i, s: (i, 0, 0)),
                pl.BlockSpec((1, visible, width), lambda i, s: (i, 0, 0)),
            ],
        ),
        out_shape=[sds(patches.shape, BF16), sds(out_grad.shape, BF16)],
        compiler_params=params(),
        name="scatter",
    )(core_arr, keep_rows, token_rows, token_other, layer_rows, layer_other)

    def reduce_rows(mine, other):
        total = mine.astype(F32) + swap(other).astype(F32)
        columns = total.shape[1]
        share = width // dp_count
        for bit in range(dp_bits):
            own_bit = (dp_index >> bit) & 1
            partners = [(d, d ^ (1 << bit)) for d in range(dp_count)]
            parted = total.reshape(-1, 2, share, columns)
            keep = lax.dynamic_index_in_dim(parted, own_bit, 1, keepdims=False)
            send = lax.dynamic_index_in_dim(parted, 1 - own_bit, 1, keepdims=False)
            moved = lax.ppermute(send.astype(BF16), "dp", partners)
            total = (keep + moved.astype(F32)).reshape(-1, columns)
        return total

    og_chunks = [lax.dynamic_slice_in_dim(grad_flat, (core * CHUNKS + c) * rows, rows, 0) for c in both]
    down_grad = weight_grad(og_chunks, [m[2] for m in mlps], units, "down_grad")
    up_grad = weight_grad([m[1] for m in mlps], [m[3] for m in mlps], units, "up_grad")
    down_sum = reduce_rows(down_grad[:, :units], down_grad[:, units:]).T
    up_sum = reduce_rows(up_grad[:, :units], up_grad[:, units:])
    attn_grads = [
        weight_grad([h[1] for h in heads], [b[2][j] for b in backs], chip_width, f"qkv_grad{j}") for j in range(3)
    ] + [weight_grad([b[1] for b in backs], [h[4] for h in heads], chip_width, "proj_grad")]
    attn_sum = reduce_rows(
        jnp.concatenate([g[:, :heads_width] for g in attn_grads], axis=1),
        jnp.concatenate([g[:, heads_width:] for g in attn_grads], axis=1),
    )
    qkv_sum = attn_sum[:, :n_qkvb].reshape(-1, 3, heads_width)
    proj_sum = attn_sum[:, n_qkvb:].T

    upb_part = mlps[0][6] + mlps[1][6]
    qkvb_part = backs[0][5] + backs[1][5]
    upb_chip = jnp.where(core == 0, upb_part, jnp.roll(upb_part, units, axis=1)).reshape(2, units)
    qkvb_chip = jnp.where(core == 0, qkvb_part, jnp.roll(qkvb_part, heads_width, axis=1))
    qkvb_flat = jnp.pad(qkvb_chip.reshape(-1), (0, 2 * width - 3 * chip_width)).reshape(2, width)
    packed = jnp.concatenate(
        [
            backs[0][4][:4] + backs[1][4][:4],
            tails[0][1][:2] + tails[1][1][:2],
            upb_chip.reshape(-1, width),
            qkvb_flat,
        ],
        axis=0,
    )
    packed = jnp.pad(packed, ((0, (-packed.shape[0]) % 8), (0, 0)))
    sums = small_sums(packed, dp_bits)
    n_up = chip_units // width
    up_rows = sums[6 : 6 + n_up].reshape(2, units)
    up_bias_sum = lax.dynamic_index_in_dim(up_rows, core, 0, keepdims=False)
    qkv_rows = sums[6 + n_up : 8 + n_up].reshape(-1)[: 3 * chip_width].reshape(3, 2, heads_width)
    qkv_bias_sum = lax.dynamic_index_in_dim(qkv_rows, core, 1, keepdims=False)
    return (
        layer_out, patches_grad, sums[4], sums[5], qkv_sum, qkv_bias_sum, proj_sum, sums[2],
        sums[0], sums[1], up_sum, up_bias_sum, down_sum, sums[3],
    )


def solution(mesh):
    return jax.shard_map(
        functools.partial(local, dp_count=mesh.shape["dp"], mp_count=mesh.shape["mp"]),
        mesh=mesh,
        in_specs=(
            P("dp", None, None), P("dp", None), P(), P(), P(None, None, "mp"), P(None, "mp"),
            P("mp", None), P(), P(), P(), P(None, "mp"), P("mp"), P("mp", None), P(),
            P("dp", None, None),
        ),
        out_specs=(
            P("dp", None, None), P("dp", None, None), P(), P(), P("dp", None, "mp"), P(None, "mp"),
            P("mp", "dp"), P(), P(), P(), P("dp", "mp"), P("mp"), P("mp", "dp"), P(),
        ),
        check_vma=False,
    )
```
